256 devices in a mesh: dp: 16 (over y, x), expert: 16 (over z, core).
Axes of the slice: x: 4, y: 4, z: 8, core: 2. Of those that a mesh axis runs over, the one named last changes fastest.
Arguments:
- tokens: bfloat16 [4096, 4096], P('dp', 'expert'), may hold values from -6 to 6
- routing: int32 [4096, 2], P('dp'), may hold values from 0 to 15, all different within a row; in each aligned block of 256 rows (0 to 255, 256 to 511, ...) at most 48 rows name the same one
- gate_weight: bfloat16 [4096, 16], P('expert'), may hold values from -0.09375 to 0.09375
- expert_in: bfloat16 [16, 4096, 8192], P('dp', None, 'expert'), may hold values from -0.09375 to 0.09375
- expert_out: bfloat16 [16, 8192, 4096], P('dp', 'expert'), may hold values from -0.75 to 0.75
Outputs:
- mixed: bfloat16 [4096, 4096], P('dp', 'expert')
The draws below stay inside these ranges and needn't reach their ends.
Inputs may be any that keep to these rules, and one draw needn't show every extreme that they name: `routing`: each row names two different experts. Within the 256 rows of one group, no expert is named by more than 48 rows, a bound that some block reaches.
All inputs are finite; a program needn't handle non-finite values.
Results may differ from the reference program's by a relative error of at most 0.02.
Values may be sent and summed in bfloat16 or wider, within the bound.
No kernel may reach another device: no remote copies, remote signals or barrier semaphores. Data moves between devices by JAX's collectives and lax.ppermute only.
A program may use at most 64 MiB of HBM per device.

```python
import math
import jax
import jax.numpy as jnp
import numpy as np
from jax import lax

D = 4096
FF = 8192
GROUP = 256
EXPERTS = 16
CAP = 48
TOKENS = 4096
N_DP = 16
N_EXPERT = 16


def strengthened(result, rng, source, target, blocks, factor):
    owner, partner = [(jnp.arange(result.shape[position]) // (result.shape[position] // blocks)).reshape([-1 if axis == position else 1 for axis in range(result.ndim)]) for position in (source, target)]
    chosen = jax.random.permutation(rng, blocks)[partner]
    strong = (owner == chosen) | (owner == (partner + blocks // 2) % blocks)
    return jnp.where(strong, factor * result, result)


def shard_levels(rng, shape, pieces, low, high):
    def one(position, blocks):
        heights = jax.random.uniform(jax.random.fold_in(jax.random.fold_in(rng, 6), position), (blocks,), jnp.float32, low / len(pieces), high / len(pieces))
        return jnp.repeat(jnp.exp(heights), shape[position] // blocks).reshape((-1,) + (1,) * (len(shape) - position - 1))

    factor_of = one(*pieces[0])
    for cut in pieces[1:]:
        factor_of = factor_of * one(*cut)
    return factor_of


def assign_block(stream_key, own, number, rows, count, top, bound, slope):
    sequence = jax.random.permutation(stream_key, count)
    crowded, ordinary = portions_of(count, rows * top, bound, slope, True), portions_of(count, rows * top, bound, slope, False)
    places = jnp.arange(count)

    def named(sizes, turn):
        used = int((sizes > 0).sum())
        fixed = max(1, used // 4)
        passed = fixed + (places - fixed + turn * (used - fixed)) % max(1, count - fixed)
        return jnp.zeros((count,), jnp.int32).at[sequence[jnp.where(places < fixed, places, passed)]].set(jnp.asarray(sizes, jnp.int32))

    sizes = jnp.where(number % 4 == 0, named(crowded, number // 4), named(ordinary, number - number // 4 - 1))
    mixed = jax.random.permutation(jax.random.fold_in(own, 3), count)
    donor, sink = mixed[0:count // 2 * 2:2], mixed[1:count // 2 * 2:2]
    room = jnp.minimum(sizes[donor] - 1, bound - sizes[sink]) // 2
    room = jnp.where((donor == sequence[0]) | (sink == sequence[0]) | (sizes[sink] == 0), 0, jnp.maximum(room, 0))
    passed = jax.random.randint(jax.random.fold_in(own, 4), (count // 2,), 0, 1 << 20) % (room + 1)
    sizes = sizes.at[donor].add(-passed).at[sink].add(passed)
    items = jnp.searchsorted(jnp.cumsum(sizes), jnp.arange(rows * top), side="right").astype(jnp.int32)
    table = items.reshape(top, rows).T
    table = table[jax.random.permutation(jax.random.fold_in(own, 1), rows)]
    turn = jax.random.randint(jax.random.fold_in(own, 2), (rows, 1), 0, top)
    return jnp.take_along_axis(table, (jnp.arange(top)[None, :] + turn) % top, axis=1)


def portions_of(count, total, most, slope, full):
    weights = [(1 << 20) // math.isqrt(grade ** slope) + 1 for grade in range(1, count + 1)]
    largest = most if full else min(most, max(-(-total // count), total * weights[0] // sum(weights)))
    least = 1 if total - largest >= count - 1 else 0
    counts, surplus = [largest] + [least] * (count - 1), total - largest - least * (count - 1)
    while surplus > 0:
        candidates = [i for i in range(1, count) if counts[i] < largest] or [i for i in range(1, count) if counts[i] < most]
        whole, left = sum([weights[i] for i in candidates]), surplus
        for i in candidates:
            more = min(most - counts[i], max(1, left * weights[i] // whole), surplus)
            counts[i] = counts[i] + more
            surplus = surplus - more
    return np.array(counts)


def centred(rng, dims, deviation, most, shards=(), kind=jnp.bfloat16):
    result = deviation * jax.random.normal(rng, dims, jnp.float32)
    if shards:
        result = result * shard_levels(rng, dims, shards, -0.22, 0.18)
    return jnp.clip(result, -most, most).astype(kind)


def noise_with(key, shape, deviation, bound, shards, heavy, kind=jnp.bfloat16):
    array = deviation * jax.random.normal(key, shape, jnp.float32)
    if shards:
        array = array * shard_levels(key, shape, shards, -0.22, 0.18)
    return jnp.clip(strengthened(array, jax.random.fold_in(key, 3), *heavy), -bound, bound).astype(kind)


def setup_inputs(seed: int = 0) -> dict:
    streams_of = jax.random.split(jax.random.key(seed), 6)
    tokens = centred(streams_of[0], (TOKENS, D), 1.0, 6.0, ((0, 16), (1, 16)))
    routing_keys = jax.random.split(jax.random.fold_in(streams_of[1], 1), TOKENS // GROUP)
    routing_turns = jax.random.permutation(jax.random.fold_in(streams_of[1], 3), TOKENS // GROUP)
    routing = jax.vmap(lambda own, number: assign_block(jax.random.fold_in(streams_of[1], 2), own, number, GROUP, EXPERTS, 2, CAP, 2))(routing_keys, routing_turns).reshape((TOKENS, 2))
    gate_weight = centred(streams_of[2], (D, EXPERTS), D ** -0.5, 0.09375, ((0, 16),))
    expert_in = centred(streams_of[3], (EXPERTS, D, FF), D ** -0.5, 0.09375, ((0, 16), (2, 16)))
    expert_out = noise_with(streams_of[4], (EXPERTS, FF, D), (FF // 64) ** -0.5, 0.75, ((0, 16), (1, 16)), (1, 2, 16, 2.0))
    return {"tokens": tokens, "routing": routing, "gate_weight": gate_weight, "expert_in": expert_in, "expert_out": expert_out}


def slot_table(grouped):
    order = jnp.transpose(grouped, (0, 2, 1)).reshape(grouped.shape[0], -1)
    onehot = (order[:, :, None] == jnp.arange(EXPERTS, dtype=jnp.int32)[None, None, :]).astype(jnp.int32)
    before = jnp.cumsum(onehot, axis=1) - onehot
    slot_flat = jnp.sum(before * onehot, axis=-1).astype(jnp.int32)
    return jnp.transpose(slot_flat.reshape(grouped.shape[0], 2, -1), (0, 2, 1))


def reference(tokens, routing, gate_weight, expert_in, expert_out):
    logits = jnp.dot(tokens, gate_weight, preferred_element_type=jnp.float32)
    raised = jnp.exp(logits)
    softmax_all = raised / jnp.sum(raised, axis=-1, keepdims=True)
    chosen = jnp.take_along_axis(softmax_all, routing, axis=1).astype(jnp.bfloat16)
    grouped = routing.reshape(N_DP, GROUP, 2)
    slot_index = slot_table(grouped)
    group_ids = jnp.broadcast_to(jnp.arange(N_DP, dtype=jnp.int32)[:, None, None], (N_DP, GROUP, 2))
    token_rows = jnp.broadcast_to(tokens.reshape(N_DP, GROUP, 1, D), (N_DP, GROUP, 2, D))
    buffer = jnp.zeros((EXPERTS, N_DP, CAP, D), jnp.bfloat16)
    buffer = buffer.at[grouped, group_ids, slot_index].set(token_rows)
    width_block = FF // N_EXPERT

    def run_expert(packed):
        rows_in, weight_in, weight_out = packed
        flat_rows = rows_in.reshape(N_DP * CAP, D)
        hidden = jax.nn.gelu(jnp.dot(flat_rows, weight_in, preferred_element_type=jnp.float32), approximate=True).astype(jnp.bfloat16)

        def add_block(index, running):
            start = (index * width_block).astype(jnp.int32)
            left = lax.dynamic_slice_in_dim(hidden, start, width_block, 1)
            right = lax.dynamic_slice_in_dim(weight_out, start, width_block, 0)
            term = jnp.dot(left, right, preferred_element_type=jnp.float32).astype(jnp.bfloat16)
            term = lax.optimization_barrier(term)
            return running + term.astype(jnp.float32)

        summed = lax.fori_loop(0, N_EXPERT, add_block, jnp.zeros((N_DP * CAP, D), jnp.float32))
        return summed.astype(jnp.bfloat16).reshape(N_DP, CAP, D)

    expert_result = lax.map(run_expert, (buffer, expert_in, expert_out))
    picked = expert_result[grouped, group_ids, slot_index]
    weights = chosen.reshape(N_DP, GROUP, 2, 1).astype(jnp.float32)
    mixed = jnp.sum(picked.astype(jnp.float32) * weights, axis=2)
    return mixed.reshape(TOKENS, D).astype(jnp.bfloat16)
```

```python
import jax
import jax.numpy as jnp
from jax import lax
from jax.sharding import Mesh
from jax.sharding import PartitionSpec as P


ZC = ("z", "c")
NZ = 8


def ring(value):
    pairs = []
    for z in range(NZ):
        pairs.append((2 * z, 2 * ((z + 1) % NZ)))
        pairs.append((2 * z + 1, 2 * ((z - 1) % NZ) + 1))
    return lax.ppermute(value, ZC, pairs)


def swap(value):
    return lax.ppermute(value, "c", [(0, 1), (1, 0)])


def shards(tokens, routing, gate_weight, expert_in, expert_out):
    group_size, width = tokens.shape
    experts = gate_weight.shape[1]
    dp_count = lax.axis_size("dp")
    capacity = 3 * group_size // dp_count
    rows = experts * capacity
    weight_in = expert_in[0]
    weight_out = expert_out[0]
    z = lax.axis_index("z")
    c = lax.axis_index("c")
    sign = 1 - 2 * c
    weight_out_p = swap(weight_out)

    part = lax.dot_general(
        gate_weight, tokens, (((0,), (1,)), ((), ())), preferred_element_type=jnp.float32
    )
    high = part.astype(jnp.bfloat16)
    low = (part - high.astype(jnp.float32)).astype(jnp.bfloat16)

    picks = routing.T
    order = picks.reshape(1, 2 * group_size)
    labels = lax.broadcasted_iota(jnp.int32, (experts, 2 * group_size), 0)
    onehot = (labels == order).astype(jnp.bfloat16)
    earlier = (
        lax.broadcasted_iota(jnp.int32, (2 * group_size, 2 * group_size), 0)
        < lax.broadcasted_iota(jnp.int32, (2 * group_size, 2 * group_size), 1)
    ).astype(jnp.bfloat16)
    before = jnp.dot(onehot, earlier, preferred_element_type=jnp.float32)
    slot = jnp.sum(before * onehot.astype(jnp.float32), axis=0, keepdims=True).astype(jnp.int32)
    target = (order * capacity + slot).reshape(2, group_size)
    row_ids = lax.broadcasted_iota(jnp.int32, (rows, group_size), 0)
    first_hit = row_ids == target[0:1]
    second_hit = row_ids == target[1:2]
    assign = jnp.logical_or(first_hit, second_hit).astype(jnp.bfloat16)
    outgoing = jnp.dot(assign, tokens, preferred_element_type=jnp.float32)
    outgoing = outgoing.astype(jnp.bfloat16).reshape(experts, capacity, width)
    incoming = lax.all_to_all(outgoing, "dp", split_axis=0, concat_axis=0, tiled=True)

    chunk = jnp.concatenate([incoming.reshape(rows, width), high, low], axis=0)

    state = {"acc": jnp.zeros((rows, weight_in.shape[1]), jnp.float32), "logits": jnp.zeros((experts, group_size), jnp.float32)}

    def use(block, zz, cc):
        start = (((zz + 2 * NZ) % NZ) * 2 + cc) * width
        weight = lax.dynamic_slice_in_dim(weight_in, start, width, 0)
        state["acc"] = state["acc"] + jnp.dot(block[:rows], weight, preferred_element_type=jnp.float32)
        state["logits"] = (
            state["logits"]
            + block[rows : rows + experts].astype(jnp.float32)
            + block[rows + experts :].astype(jnp.float32)
        )

    a = chunk
    b = swap(chunk)
    use(a, z, c)
    use(b, z, 1 - c)
    for step in range(1, 5):
        a = ring(a)
        use(a, z - sign * step, c)
        if step < 4:
            b = ring(b)
            use(b, z - sign * step, 1 - c)
        use(swap(a), z + sign * step, 1 - c)
        if step < 4:
            use(swap(b), z + sign * step, c)

    hidden = jax.nn.gelu(state["acc"], approximate=True).astype(jnp.bfloat16)
    hidden_p = swap(hidden)

    def partial(zz, cc):
        start = (((zz + 2 * NZ) % NZ) * 2 + cc) * width
        own = jnp.dot(
            hidden, lax.dynamic_slice_in_dim(weight_out, start, width, 1), preferred_element_type=jnp.float32
        )
        other = jnp.dot(
            hidden_p, lax.dynamic_slice_in_dim(weight_out_p, start, width, 1), preferred_element_type=jnp.float32
        )
        return lax.optimization_barrier(own + other)

    ra = partial(z + 4 * sign, c).astype(jnp.bfloat16)
    rb = partial(z + 3 * sign, 1 - c).astype(jnp.bfloat16)
    for step in range(1, 4):
        ra = (ring(ra).astype(jnp.float32) + partial(z + sign * (4 - step), c)).astype(jnp.bfloat16)
        rb = ring(rb)
        if step < 3:
            rb = (rb.astype(jnp.float32) + partial(z + sign * (3 - step), 1 - c)).astype(jnp.bfloat16)
    total = ring(ra).astype(jnp.float32) + partial(z, c) + swap(rb).astype(jnp.float32)
    processed = total.astype(jnp.bfloat16).reshape(experts, capacity, width)
    returned = lax.all_to_all(processed, "dp", split_axis=0, concat_axis=0, tiled=True)

    raised = jnp.exp(state["logits"])
    probs = raised / jnp.sum(raised, axis=0, keepdims=True)
    expert_ids = lax.broadcasted_iota(jnp.int32, (experts, group_size), 0)
    chosen = [
        jnp.sum(jnp.where(expert_ids == picks[k : k + 1], probs, 0.0), axis=0, keepdims=True).astype(jnp.bfloat16)
        for k in range(2)
    ]
    zero = jnp.zeros((), jnp.bfloat16)
    combine = jnp.where(first_hit, chosen[0], zero) + jnp.where(second_hit, chosen[1], zero)
    mixed = lax.dot_general(
        combine, returned.reshape(rows, width), (((0,), (0,)), ((), ())), preferred_element_type=jnp.float32
    )
    return mixed.astype(jnp.bfloat16)


def solution(mesh):
    torus = Mesh(mesh.devices.reshape(mesh.shape["dp"], NZ, 2), ("dp", "z", "c"))
    placed = (
        P("dp", ZC),
        P("dp", None),
        P(ZC, None),
        P("dp", None, ZC),
        P("dp", ZC, None),
    )
    return jax.shard_map(
        shards, mesh=torus, in_specs=placed, out_specs=P("dp", ZC), check_vma=False
    )
```
